32 devices in a mesh: group: 2 (over y), cp: 8 (over z, x), hd: 2 (over core).
Axes of the slice: x: 2, y: 2, z: 4, core: 2. Of those that a mesh axis runs over, the one named last changes fastest.
Arguments:
- doc_lengths: int32 [8], P('group'), parts along dimension 0, may hold values from 1 to 384, 1024 in all
- queries: bfloat16 [2048, 4096], P(('group', 'cp'), 'hd'), parts along dimension 0, may hold values from -52 to 52
- key_states: bfloat16 [2048, 1024], P(('group', 'cp'), 'hd'), parts along dimension 0, may hold values from -4 to 4
- value_head_states: bfloat16 [2048, 1024], P(('group', 'cp'), 'hd'), parts along dimension 0, may hold values from -6 to 6
- out_grad: bfloat16 [2048, 4096], P(('group', 'cp'), 'hd'), parts along dimension 0, may hold values from -6 to 6
Outputs:
- attended: bfloat16 [2048, 4096], P(('group', 'cp'), 'hd'), parts along dimension 0
- grad_queries: bfloat16 [2048, 4096], P(('group', 'cp'), 'hd'), parts along dimension 0
- grad_keys: bfloat16 [2048, 1024], P(('group', 'cp'), 'hd'), parts along dimension 0
- grad_values: bfloat16 [2048, 1024], P(('group', 'cp'), 'hd'), parts along dimension 0
The draws below stay inside these ranges and needn't reach their ends.
There are 2 independent parts, one for each index of `group`. The reference program is written for one: setup_inputs(seed, part) draws one part's arguments, and reference() takes and returns one part's arrays. A program takes and returns all parts, laid end to end along the dimension named above; each array names one. Nothing has to cross between parts.
Inputs may be any that keep to these rules, and one draw needn't show every extreme that they name: `doc_lengths`: documents lie end to end in token order; their lengths sum to 1024.
All inputs are finite; a program needn't handle non-finite values.
Results may differ from the reference program's by a relative error of at most 0.028.
Values may be sent and summed in bfloat16 or wider, within the bound.
A program may use at most 64 MiB of HBM per device.

```python
import math
import jax
import jax.numpy as jnp
import numpy as np
from jax import lax

QUERY_HEADS_COUNT = 32
KEY_VALUE_HEADS = 8
HEAD_SIZE = 128
TOK_DEV = 128
REACH = 3
WINDOW_TOKENS = 1024
MAXDOC = 384
DOCS = 4
N_CP = 8


def starting_keys(key):
    array_extent = (WINDOW_TOKENS, KEY_VALUE_HEADS * HEAD_SIZE)
    sampled_values = jax.random.truncated_normal(jax.random.fold_in(key, 12), -4.0, 4.0, array_extent, jnp.float32)
    return sampled_values


def draw_key_states(key, part):
    sampled_values = starting_keys(key)
    return sampled_values.astype(jnp.bfloat16)


def draw_queries(key, part):
    array_extent = (WINDOW_TOKENS, QUERY_HEADS_COUNT * HEAD_SIZE)
    sampled_values = jax.random.truncated_normal(jax.random.fold_in(key, 13), -4.0, 4.0, array_extent, jnp.float32)
    return sampled_values.astype(jnp.bfloat16)


def level_of(stream_key, shape, pieces, smallest, high):
    factor_of, own = 1.0, jax.random.fold_in(stream_key, 6)
    for dim, shards_of in pieces:
        draws = jnp.exp(jax.random.uniform(jax.random.fold_in(own, dim), (shards_of,), jnp.float32, smallest / len(pieces), high / len(pieces)))
        factor_of = factor_of * jnp.repeat(draws, shape[dim] // shards_of).reshape([-1 if axis == dim else 1 for axis in range(len(shape))])
    return factor_of


def length_profile(count, total, bound, slope):
    loads = [(1 << 20) // math.isqrt(grade ** slope) + 1 for grade in range(2, count + 1)]
    rest, given = total - bound - (count - 1), [1] * (count - 1)
    while rest > 0:
        candidates = [i for i in range(count - 1) if given[i] < bound]
        pool, budget = sum([loads[i] for i in candidates]), rest
        for i in candidates:
            extra = min(bound - given[i], max(1, budget * loads[i] // pool), rest)
            given[i] = given[i] + extra
            rest = rest - extra
    return np.array([bound] + given)


def uneven_parts(own_key, amount, total, limit, skew):
    if amount == 2:
        one = jax.random.randint(own_key, (), max(1, total - limit), min(limit, total - 1) + 1)
        return jnp.stack([one, total - one])
    lengths = jnp.asarray(length_profile(amount, total, limit, skew), jnp.int32)
    twos = (amount - 1) // 2
    giver, receiver = lengths[1:1 + 2 * twos:2], lengths[2:2 + 2 * twos:2]
    margin = jnp.minimum(giver - 1, limit - receiver)
    passed = jax.random.randint(jax.random.fold_in(own_key, 1), (twos,), 0, 1 << 20) % (margin + 1)
    lengths = lengths.at[1:1 + 2 * twos:2].set(giver - passed).at[2:2 + 2 * twos:2].set(receiver + passed)
    return lengths[jax.random.permutation(jax.random.fold_in(own_key, 2), amount)]


def scatter_about(rng, dims, scale, bound, pieces=(), kind=jnp.bfloat16):
    values = jax.random.normal(rng, dims, jnp.float32) * scale
    if len(pieces) > 0:
        values = level_of(rng, dims, pieces, -0.22, 0.18) * values
    return jnp.clip(values, min=-bound, max=bound).astype(kind)


def setup_inputs(seed: int = 0, part: int = 0) -> dict:
    arg_keys = jax.random.split(jax.random.key(seed), 6)
    own_keys = jax.random.split(jax.random.fold_in(arg_keys[5], part), 6)
    return {
        "doc_lengths": uneven_parts(own_keys[0], DOCS, WINDOW_TOKENS, MAXDOC, 2).astype(jnp.int32),
        "queries": draw_queries(jax.random.fold_in(jax.random.fold_in(arg_keys[5], part), 71), part),
        "key_states": draw_key_states(jax.random.fold_in(jax.random.fold_in(arg_keys[5], part), 71), part),
        "value_head_states": scatter_about(own_keys[3], (WINDOW_TOKENS, KEY_VALUE_HEADS * HEAD_SIZE), 1.0, 6.0, ((0, 8), (1, 2))),
        "out_grad": scatter_about(own_keys[4], (WINDOW_TOKENS, QUERY_HEADS_COUNT * HEAD_SIZE), 1.0, 6.0, ((0, 8), (1, 2))),
    }


masked_score = -1e+30

def document_ids(doc_lengths, positions):
    ends = jnp.cumsum(doc_lengths).astype(jnp.int32)
    counted = lax.optimization_barrier(jnp.sum((ends[None, :] <= positions[:, None]).astype(jnp.int32), axis=1)).astype(jnp.int32)
    return jnp.where(positions < 0, jnp.int32(-1), counted)

def attend(queries, key_rows, value_rows, out_grad, allowed):
    tok_rows = queries.shape[0]
    window_rows = key_rows.shape[0]
    head_kv = key_rows.shape[1] // HEAD_SIZE
    group_size = queries.shape[1] // key_rows.shape[1]
    score_scale = 1.0 / math.sqrt(HEAD_SIZE)
    query_heads = queries.reshape(tok_rows, head_kv, group_size, HEAD_SIZE).astype(jnp.float32)
    key_heads = key_rows.reshape(window_rows, head_kv, HEAD_SIZE).astype(jnp.float32)
    value_heads = value_rows.reshape(window_rows, head_kv, HEAD_SIZE).astype(jnp.float32)
    grad_heads = out_grad.reshape(tok_rows, head_kv, group_size, HEAD_SIZE).astype(jnp.float32)
    scores = jnp.einsum('qhgd,khd->hgqk', query_heads, key_heads) * score_scale
    scores = jnp.where(allowed, scores, masked_score)
    row_max = lax.optimization_barrier(jnp.max(scores, axis=-1, keepdims=True))
    weights_raw = jnp.exp(scores - row_max)
    probs = weights_raw / lax.optimization_barrier(jnp.sum(weights_raw, axis=-1, keepdims=True))
    probs_low = probs.astype(jnp.bfloat16).astype(jnp.float32)
    attended = jnp.einsum('hgqk,khd->qhgd', probs_low, value_heads).astype(jnp.bfloat16)
    delta = lax.optimization_barrier(jnp.sum(grad_heads * attended.astype(jnp.float32), axis=-1)).transpose(1, 2, 0)
    grad_value = jnp.einsum('hgqk,qhgd->khd', probs_low, grad_heads)
    grad_probs = jnp.einsum('qhgd,khd->hgqk', grad_heads, value_heads)
    grad_scores = (probs * (grad_probs - delta[..., None])).astype(jnp.bfloat16).astype(jnp.float32)
    grad_query = (jnp.einsum('hgqk,khd->qhgd', grad_scores, key_heads) * score_scale).astype(jnp.bfloat16)
    grad_key = jnp.einsum('hgqk,qhgd->khd', grad_scores, query_heads) * score_scale
    return (attended.reshape(tok_rows, -1), grad_query.reshape(tok_rows, -1), grad_key.reshape(window_rows, -1), grad_value.reshape(window_rows, -1))

def reference(doc_lengths, queries, key_states, value_head_states, out_grad):
    tok_rows = TOK_DEV
    window_rows = (REACH + 1) * tok_rows
    pad_rows = REACH * tok_rows
    columns = key_states.shape[1]
    padding = jnp.zeros((pad_rows, columns), key_states.dtype)
    keys_padded = jnp.concatenate([padding, key_states], axis=0)
    values_padded = jnp.concatenate([padding, value_head_states], axis=0)
    empty = jnp.zeros((pad_rows + WINDOW_TOKENS, columns), jnp.float32)

    def block_step(carry, block_index):
        sum_keys, sum_values = carry
        row_start = (block_index * tok_rows).astype(jnp.int32)
        query_block = lax.dynamic_slice_in_dim(queries, row_start, tok_rows, 0)
        grad_block = lax.dynamic_slice_in_dim(out_grad, row_start, tok_rows, 0)
        key_block = lax.dynamic_slice_in_dim(keys_padded, row_start, window_rows, 0)
        value_block = lax.dynamic_slice_in_dim(values_padded, row_start, window_rows, 0)
        query_pos = row_start + lax.iota(jnp.int32, tok_rows)
        key_pos = row_start - pad_rows + lax.iota(jnp.int32, window_rows)
        query_ids = document_ids(doc_lengths, query_pos)
        key_ids = document_ids(doc_lengths, key_pos)
        allowed = (query_ids[:, None] == key_ids[None, :]) & (key_pos[None, :] <= query_pos[:, None])
        attended, grad_query, grad_key, grad_value = attend(query_block, key_block, value_block, grad_block, allowed)
        old_keys = lax.dynamic_slice_in_dim(sum_keys, row_start, window_rows, 0)
        old_values = lax.dynamic_slice_in_dim(sum_values, row_start, window_rows, 0)
        sum_keys = lax.dynamic_update_slice_in_dim(sum_keys, old_keys + grad_key, row_start, 0)
        sum_values = lax.dynamic_update_slice_in_dim(sum_values, old_values + grad_value, row_start, 0)
        return ((sum_keys, sum_values), (attended, grad_query))
    (sum_keys, sum_values), (outs, grads) = lax.scan(block_step, (empty, empty), jnp.arange(N_CP, dtype=jnp.int32))
    attended = outs.reshape(WINDOW_TOKENS, -1)
    grad_queries = grads.reshape(WINDOW_TOKENS, -1)
    grad_keys = sum_keys[pad_rows:].astype(jnp.bfloat16)
    grad_values = sum_values[pad_rows:].astype(jnp.bfloat16)
    return (attended, grad_queries, grad_keys, grad_values)
```

```python
import functools
import math

import jax
import jax.numpy as jnp
from jax import lax
from jax.experimental import pallas as pl
from jax.experimental.pallas import tpu as pltpu
from jax.sharding import PartitionSpec as P

HEAD = 128
REACH = 3
MASKED = -1e30
MESH = pl.DeviceIdType.MESH
A, B, C, D = range(4)


def kernel(
    n, docs, doc_ref, q_hbm, k_hbm, v_hbm, do_hbm, o_hbm, gq_hbm, gk_hbm, gv_hbm,
    kv, qb, db, ob, gqb, own, mid, part, back, outkv, bias,
    kv_sem, q_sem, out_sem, gout_sem, fs_sem, fr_sem, bs_sem, br_sem,
):
    tok = q_hbm.shape[0]
    heads = k_hbm.shape[1] // HEAD
    group = q_hbm.shape[1] // k_hbm.shape[1]
    me = lax.axis_index("cp")
    odd = lax.rem(me, 2)
    is_odd = odd == 1
    is_even = odd == 0
    partner = me + 1 - 2 * odd
    diag = me - 1 + 2 * odd
    own_rows = pl.ds(REACH * tok, tok)

    def rows(dist):
        return pl.ds((REACH - dist) * tok, tok)

    def cols(h):
        return pl.ds(h * HEAD, HEAD)

    kv_loads = []
    for g in range(heads):
        kv_loads.append([
            pltpu.make_async_copy(src.at[:, cols(g)], kv.at[g, t, own_rows], kv_sem.at[g, t])
            for t, src in enumerate((k_hbm, v_hbm))
        ])
        for c in kv_loads[g]:
            c.start()
    q_loads = []
    for h in range(heads * group):
        q_loads.append([
            pltpu.make_async_copy(q_hbm.at[:, cols(h)], qb.at[h], q_sem.at[0, h]),
            pltpu.make_async_copy(do_hbm.at[:, cols(h)], db.at[h], q_sem.at[1, h]),
        ])
        for c in q_loads[h]:
            c.start()

    barrier = pltpu.get_barrier_semaphore()
    offsets = (-2, -1, 1, 2)
    for off in offsets:
        @pl.when((me + off >= 0) & (me + off < n))
        def _():
            pl.semaphore_signal(barrier, inc=1, device_id={"cp": me + off}, device_id_type=MESH)
    behind = jnp.minimum(me, 2)
    ahead = jnp.minimum(n - 1 - me, 2)
    pl.semaphore_wait(barrier, behind + ahead)

    def fwd(kind, g, src_rows, dst_rows, to):
        return pltpu.make_async_remote_copy(
            src_ref=kv.at[g, :, src_rows], dst_ref=kv.at[g, :, dst_rows],
            send_sem=fs_sem.at[kind, g], recv_sem=fr_sem.at[kind, g],
            device_id={"cp": to}, device_id_type=MESH,
        )

    def fwd_a(g):
        return fwd(A, g, own_rows, rows(1), partner)

    def fwd_b(g):
        return fwd(B, g, own_rows, rows(2), me + 2)

    def fwd_c_out(g):
        return fwd(C, g, rows(2), pl.ds(odd * 2 * tok, tok), partner)

    def fwd_c_in(g):
        return fwd(C, g, rows(2), pl.ds((1 - odd) * 2 * tok, tok), partner)

    def fwd_d(g):
        return fwd(D, g, rows(2), rows(3), diag)

    has_a_out = is_even
    has_a_in = is_odd
    has_b_out = me + 2 < n
    has_b_in = me >= 2
    has_c = me >= 2
    has_d_out = is_odd & (me >= 3) & (me + 1 < n)
    has_d_in = is_even & (me >= 4)

    for g in range(heads):
        for c in kv_loads[g]:
            c.wait()
        @pl.when(has_b_out)
        def _():
            fwd_b(g).start()
        @pl.when(has_a_out)
        def _():
            fwd_a(g).start()

    for dist in range(1, REACH + 1):
        @pl.when(me < dist)
        def _():
            kv[:, :, (REACH - dist) * tok:(REACH - dist + 1) * tok, :] = jnp.zeros(
                (heads, 2, tok, HEAD), kv.dtype)

    window = (REACH + 1) * tok
    key_pos = (me - REACH) * tok + lax.broadcasted_iota(jnp.int32, (window, tok), 0)
    query_pos = me * tok + lax.broadcasted_iota(jnp.int32, (window, tok), 1)

    end = jnp.int32(0)
    crossed = jnp.zeros((window, tok), jnp.int32)
    def count(d, carry):
        end, crossed = carry
        end = end + doc_ref[d]
        return end, crossed + jnp.where((key_pos < end) & (query_pos >= end), 1, 0)
    if docs <= 8:
        for d in range(docs):
            end, crossed = count(d, (end, crossed))
    else:
        end, crossed = lax.fori_loop(0, docs, count, (end, crossed))
    allowed = (crossed == 0) & (key_pos <= query_pos) & (key_pos >= 0)
    bias[...] = jnp.where(allowed, 0.0, MASKED)

    def relay(g):
        @pl.when(has_b_in)
        def _():
            fwd_b(g).wait_recv()
        @pl.when(has_d_out)
        def _():
            fwd_d(g).start()
        @pl.when(has_c)
        def _():
            fwd_c_out(g).start()

    def arrive(g):
        @pl.when(has_a_in)
        def _():
            fwd_a(g).wait_recv()
        @pl.when(has_c)
        def _():
            fwd_c_in(g).wait_recv()
        @pl.when(has_d_in)
        def _():
            fwd_d(g).wait_recv()

    def bwd(kind, g, src_rows, to):
        return pltpu.make_async_remote_copy(
            src_ref=part.at[g, :, src_rows], dst_ref=back.at[kind, g],
            send_sem=bs_sem.at[kind, g], recv_sem=br_sem.at[kind, g],
            device_id={"cp": to}, device_id_type=MESH,
        )

    def bwd_a(g):
        return bwd(A, g, rows(1), partner)

    def bwd_b(g):
        return bwd(B, g, rows(2), me - 2)

    def bwd_c(g):
        return bwd(C, g, pl.ds((1 - odd) * 2 * tok, tok), partner)

    def bwd_d(g):
        return bwd(D, g, rows(3), diag)

    score_scale = 1.0 / math.sqrt(HEAD)
    exp_scale = score_scale * math.log2(math.e)
    nt = (((1,), (1,)), ((), ()))
    step = 2 if group % 2 == 0 else 1
    width = step * tok

    out_copies = []

    def compute(g):
        keys = kv[g, 0]
        values = kv[g, 1]
        keys_t = keys.T
        values_t = values.T
        grad_k = jnp.zeros((window, HEAD), jnp.float32)
        grad_v = jnp.zeros((window, HEAD), jnp.float32)
        mask = jnp.concatenate([bias[...]] * step, axis=1)
        for s in range(group // step):
            h0 = g * group + s * step
            for h in range(h0, h0 + step):
                for c in q_loads[h]:
                    c.wait()
            qs = qb[h0:h0 + step].reshape(width, HEAD)
            ds = db[h0:h0 + step].reshape(width, HEAD)
            scores = lax.dot_general(keys, qs, nt, preferred_element_type=jnp.float32) + mask
            top = jnp.max(scores, axis=0, keepdims=True)
            raw = jnp.exp2((scores - top) * exp_scale)
            probs = raw * (1.0 / jnp.sum(raw, axis=0, keepdims=True))
            low = probs.astype(jnp.bfloat16)
            att_t = jnp.dot(values_t, low, preferred_element_type=jnp.float32)
            grad_p = lax.dot_general(values, ds, nt, preferred_element_type=jnp.float32)
            delta = jnp.sum(probs * grad_p, axis=0, keepdims=True)
            grad_s = (probs * (grad_p - delta)).astype(jnp.bfloat16)
            grad_v = grad_v + jnp.dot(low, ds, preferred_element_type=jnp.float32)
            grad_k = grad_k + jnp.dot(grad_s, qs, preferred_element_type=jnp.float32)
            gq_t = jnp.dot(keys_t, grad_s, preferred_element_type=jnp.float32) * score_scale
            for j in range(step):
                h = h0 + j
                ob[h] = att_t[:, j * tok:(j + 1) * tok].T.astype(ob.dtype)
                gqb[h] = gq_t[:, j * tok:(j + 1) * tok].T.astype(gqb.dtype)
                for t, (buf, dst) in enumerate(((ob, o_hbm), (gqb, gq_hbm))):
                    c = pltpu.make_async_copy(buf.at[h], dst.at[:, cols(h)], out_sem.at[t, h])
                    c.start()
                    out_copies.append(c)
        for t, grad in enumerate((grad_k * score_scale, grad_v)):
            part[g, t] = grad[:REACH * tok].astype(part.dtype)
            mid[g, t] = grad[tok:2 * tok]
            own[g, t] = grad[REACH * tok:]

    def give_back(g):
        @pl.when(has_d_in)
        def _():
            bwd_d(g).start()
        @pl.when(has_c)
        def _():
            bwd_c(g).start()
        @pl.when(has_a_in)
        def _():
            bwd_a(g).start()

    def collect(g):
        @pl.when(has_c)
        def _():
            bwd_c(g).wait_recv()
            mid[g] = mid[g] + back[C, g].astype(jnp.float32)
        @pl.when(has_d_out)
        def _():
            bwd_d(g).wait_recv()
            mid[g] = mid[g] + back[D, g].astype(jnp.float32)
        @pl.when(has_b_in)
        def _():
            part[g, :, tok:2 * tok] = mid[g].astype(part.dtype)
            bwd_b(g).start()

    def finish(g):
        @pl.when(has_a_out)
        def _():
            bwd_a(g).wait_recv()
            own[g] = own[g] + back[A, g].astype(jnp.float32)
        @pl.when(has_b_out)
        def _():
            bwd_b(g).wait_recv()
            own[g] = own[g] + back[B, g].astype(jnp.float32)
        outkv[g] = own[g].astype(outkv.dtype)
        for t, dst in enumerate((gk_hbm, gv_hbm)):
            c = pltpu.make_async_copy(outkv.at[g, t], dst.at[:, cols(g)], gout_sem.at[t, g])
            c.start()
            out_copies.append(c)

    relay(0)
    for g in range(heads):
        if g + 1 < heads:
            relay(g + 1)
        arrive(g)
        compute(g)
        give_back(g)
        if g >= 1:
            collect(g - 1)
        if g >= 2:
            finish(g - 2)
    collect(heads - 1)
    for g in range(max(heads - 2, 0), heads):
        finish(g)

    for g in range(heads):
        for cond, copies in (
            (has_a_out, (fwd_a,)), (has_b_out, (fwd_b,)), (has_c, (fwd_c_out, bwd_c)),
            (has_d_out, (fwd_d,)), (has_a_in, (bwd_a,)), (has_b_in, (bwd_b,)), (has_d_in, (bwd_d,)),
        ):
            @pl.when(cond)
            def _():
                for f in copies:
                    f(g).wait_send()
    for c in out_copies:
        c.wait()


def shards(doc_lengths, queries, key_states, value_head_states, out_grad):
    tok = queries.shape[0]
    heads = key_states.shape[1] // HEAD
    q_heads = queries.shape[1] // HEAD
    n = lax.axis_size("cp")
    window = (REACH + 1) * tok
    bf16, f32 = jnp.bfloat16, jnp.float32
    any_spec = pl.BlockSpec(memory_space=pl.ANY)
    dma = pltpu.SemaphoreType.DMA
    return tuple(pl.pallas_call(
        functools.partial(kernel, n, doc_lengths.shape[0]),
        out_shape=[
            jax.ShapeDtypeStruct(queries.shape, bf16),
            jax.ShapeDtypeStruct(queries.shape, bf16),
            jax.ShapeDtypeStruct(key_states.shape, bf16),
            jax.ShapeDtypeStruct(key_states.shape, bf16),
        ],
        in_specs=[pl.BlockSpec(memory_space=pltpu.SMEM)] + [any_spec] * 4,
        out_specs=[any_spec] * 4,
        scratch_shapes=[
            pltpu.VMEM((heads, 2, window, HEAD), bf16),
            pltpu.VMEM((q_heads, tok, HEAD), bf16),
            pltpu.VMEM((q_heads, tok, HEAD), bf16),
            pltpu.VMEM((q_heads, tok, HEAD), bf16),
            pltpu.VMEM((q_heads, tok, HEAD), bf16),
            pltpu.VMEM((heads, 2, tok, HEAD), f32),
            pltpu.VMEM((heads, 2, tok, HEAD), f32),
            pltpu.VMEM((heads, 2, REACH * tok, HEAD), bf16),
            pltpu.VMEM((4, heads, 2, tok, HEAD), bf16),
            pltpu.VMEM((heads, 2, tok, HEAD), bf16),
            pltpu.VMEM((window, tok), f32),
            dma((heads, 2)),
            dma((2, q_heads)),
            dma((2, q_heads)),
            dma((2, heads)),
            dma((4, heads)),
            dma((4, heads)),
            dma((4, heads)),
            dma((4, heads)),
        ],
        compiler_params=pltpu.CompilerParams(
            collective_id=0, has_side_effects=True, vmem_limit_bytes=48 * 2**20),
        name="attend",
    )(doc_lengths, queries, key_states, value_head_states, out_grad))


def solution(mesh):
    wide = P(("group", "cp"), "hd")
    return jax.shard_map(
        shards,
        mesh=mesh,
        in_specs=(P("group"), wide, wide, wide, wide),
        out_specs=(wide, wide, wide, wide),
        check_vma=False,
    )
```

```python
import functools
import math

import jax
import jax.numpy as jnp
from jax import lax
from jax.experimental import pallas as pl
from jax.experimental.pallas import tpu as pltpu
from jax.sharding import PartitionSpec as P

HEAD = 128
REACH = 3
MASKED = -1e30
MESH = pl.DeviceIdType.MESH
A, B, C, D = range(4)


def kernel(
    n, docs, doc_hbm, q_hbm, k_hbm, v_hbm, do_hbm, o_ref, gq_ref, gk_ref, gv_ref,
    kv, qb, db, own, mid, part, back, bias, doc_ref,
    doc_sem, kv_sem, q_sem, fs_sem, fr_sem, bs_sem, br_sem,
):
    tok = q_hbm.shape[0]
    heads = k_hbm.shape[1] // HEAD
    group = q_hbm.shape[1] // k_hbm.shape[1]
    me = lax.axis_index("cp")
    odd = lax.rem(me, 2)
    is_odd = odd == 1
    is_even = odd == 0
    partner = me + 1 - 2 * odd
    diag = me - 1 + 2 * odd
    own_rows = pl.ds(REACH * tok, tok)

    def rows(dist):
        return pl.ds((REACH - dist) * tok, tok)

    def cols(h):
        return pl.ds(h * HEAD, HEAD)

    doc_load = pltpu.make_async_copy(doc_hbm, doc_ref, doc_sem)
    doc_load.start()
    kv_loads = []
    for g in range(heads):
        kv_loads.append([
            pltpu.make_async_copy(src.at[:, cols(g)], kv.at[g, t, own_rows], kv_sem.at[g, t])
            for t, src in enumerate((k_hbm, v_hbm))
        ])
        for c in kv_loads[g]:
            c.start()
    q_loads = []
    for h in range(heads * group):
        q_loads.append([
            pltpu.make_async_copy(q_hbm.at[:, cols(h)], qb.at[h], q_sem.at[0, h]),
            pltpu.make_async_copy(do_hbm.at[:, cols(h)], db.at[h], q_sem.at[1, h]),
        ])
        for c in q_loads[h]:
            c.start()

    barrier = pltpu.get_barrier_semaphore()
    offsets = (-2, -1, 1, 2)
    for off in offsets:
        @pl.when((me + off >= 0) & (me + off < n))
        def _():
            pl.semaphore_signal(barrier, inc=1, device_id={"cp": me + off}, device_id_type=MESH)
    behind = jnp.minimum(me, 2)
    ahead = jnp.minimum(n - 1 - me, 2)
    pl.semaphore_wait(barrier, behind + ahead)

    def fwd(kind, g, src_rows, dst_rows, to):
        return pltpu.make_async_remote_copy(
            src_ref=kv.at[g, :, src_rows], dst_ref=kv.at[g, :, dst_rows],
            send_sem=fs_sem.at[kind, g], recv_sem=fr_sem.at[kind, g],
            device_id={"cp": to}, device_id_type=MESH,
        )

    def fwd_a(g):
        return fwd(A, g, own_rows, rows(1), partner)

    def fwd_b(g):
        return fwd(B, g, own_rows, rows(2), me + 2)

    def fwd_c_out(g):
        return fwd(C, g, rows(2), pl.ds(odd * 2 * tok, tok), partner)

    def fwd_c_in(g):
        return fwd(C, g, rows(2), pl.ds((1 - odd) * 2 * tok, tok), partner)

    def fwd_d(g):
        return fwd(D, g, rows(2), rows(3), diag)

    has_a_out = is_even
    has_a_in = is_odd
    has_b_out = me + 2 < n
    has_b_in = me >= 2
    has_c = me >= 2
    has_d_out = is_odd & (me >= 3) & (me + 1 < n)
    has_d_in = is_even & (me >= 4)

    for g in range(heads):
        for c in kv_loads[g]:
            c.wait()
        @pl.when(has_b_out)
        def _():
            fwd_b(g).start()
        @pl.when(has_a_out)
        def _():
            fwd_a(g).start()

    for dist in range(1, REACH + 1):
        @pl.when(me < dist)
        def _():
            kv[:, :, (REACH - dist) * tok:(REACH - dist + 1) * tok, :] = jnp.zeros(
                (heads, 2, tok, HEAD), kv.dtype)

    window = (REACH + 1) * tok
    key_pos = (me - REACH) * tok + lax.broadcasted_iota(jnp.int32, (window, tok), 0)
    query_pos = me * tok + lax.broadcasted_iota(jnp.int32, (window, tok), 1)

    doc_load.wait()
    end = jnp.int32(0)
    crossed = jnp.zeros((window, tok), jnp.int32)
    def count(d, carry):
        end, crossed = carry
        end = end + doc_ref[d]
        return end, crossed + jnp.where((key_pos < end) & (query_pos >= end), 1, 0)
    if docs <= 8:
        for d in range(docs):
            end, crossed = count(d, (end, crossed))
    else:
        end, crossed = lax.fori_loop(0, docs, count, (end, crossed))
    allowed = (crossed == 0) & (key_pos <= query_pos) & (key_pos >= 0)
    bias[...] = jnp.where(allowed, 0.0, MASKED)

    def relay(g):
        @pl.when(has_b_in)
        def _():
            fwd_b(g).wait_recv()
        @pl.when(has_d_out)
        def _():
            fwd_d(g).start()
        @pl.when(has_c)
        def _():
            fwd_c_out(g).start()

    def arrive(g):
        @pl.when(has_a_in)
        def _():
            fwd_a(g).wait_recv()
        @pl.when(has_c)
        def _():
            fwd_c_in(g).wait_recv()
        @pl.when(has_d_in)
        def _():
            fwd_d(g).wait_recv()

    def bwd(kind, g, src_rows, to):
        return pltpu.make_async_remote_copy(
            src_ref=part.at[g, :, src_rows], dst_ref=back.at[kind, g],
            send_sem=bs_sem.at[kind, g], recv_sem=br_sem.at[kind, g],
            device_id={"cp": to}, device_id_type=MESH,
        )

    def bwd_a(g):
        return bwd(A, g, rows(1), partner)

    def bwd_b(g):
        return bwd(B, g, rows(2), me - 2)

    def bwd_c(g):
        return bwd(C, g, pl.ds((1 - odd) * 2 * tok, tok), partner)

    def bwd_d(g):
        return bwd(D, g, rows(3), diag)

    score_scale = 1.0 / math.sqrt(HEAD)
    exp_scale = score_scale * math.log2(math.e)
    nt = (((1,), (1,)), ((), ()))
    step = 2 if group % 2 == 0 else 1
    width = step * tok

    def compute(g):
        keys = kv[g, 0]
        values = kv[g, 1]
        keys_t = keys.T
        values_t = values.T
        grad_k = jnp.zeros((window, HEAD), jnp.float32)
        grad_v = jnp.zeros((window, HEAD), jnp.float32)
        mask = jnp.concatenate([bias[...]] * step, axis=1)
        for s in range(group // step):
            h0 = g * group + s * step
            for h in range(h0, h0 + step):
                for c in q_loads[h]:
                    c.wait()
            qs = qb[h0:h0 + step].reshape(width, HEAD)
            ds = db[h0:h0 + step].reshape(width, HEAD)
            scores = lax.dot_general(keys, qs, nt, preferred_element_type=jnp.float32) + mask
            top = jnp.max(scores, axis=0, keepdims=True)
            raw = jnp.exp2((scores - top) * exp_scale)
            probs = raw * (1.0 / jnp.sum(raw, axis=0, keepdims=True))
            low = probs.astype(jnp.bfloat16)
            att_t = jnp.dot(values_t, low, preferred_element_type=jnp.float32)
            grad_p = lax.dot_general(values, ds, nt, preferred_element_type=jnp.float32)
            delta = jnp.sum(probs * grad_p, axis=0, keepdims=True)
            grad_s = (probs * (grad_p - delta)).astype(jnp.bfloat16)
            grad_v = grad_v + jnp.dot(low, ds, preferred_element_type=jnp.float32)
            grad_k = grad_k + jnp.dot(grad_s, qs, preferred_element_type=jnp.float32)
            gq_t = jnp.dot(keys_t, grad_s, preferred_element_type=jnp.float32) * score_scale
            for j in range(step):
                h = h0 + j
                o_ref[:, cols(h)] = att_t[:, j * tok:(j + 1) * tok].T.astype(o_ref.dtype)
                gq_ref[:, cols(h)] = gq_t[:, j * tok:(j + 1) * tok].T.astype(gq_ref.dtype)
        for t, grad in enumerate((grad_k * score_scale, grad_v)):
            part[g, t] = grad[:REACH * tok].astype(part.dtype)
            mid[g, t] = grad[tok:2 * tok]
            own[g, t] = grad[REACH * tok:]

    def give_back(g):
        @pl.when(has_d_in)
        def _():
            bwd_d(g).start()
        @pl.when(has_c)
        def _():
            bwd_c(g).start()
        @pl.when(has_a_in)
        def _():
            bwd_a(g).start()

    def collect(g):
        @pl.when(has_c)
        def _():
            bwd_c(g).wait_recv()
            mid[g] = mid[g] + back[C, g].astype(jnp.float32)
        @pl.when(has_d_out)
        def _():
            bwd_d(g).wait_recv()
            mid[g] = mid[g] + back[D, g].astype(jnp.float32)
        @pl.when(has_b_in)
        def _():
            part[g, :, tok:2 * tok] = mid[g].astype(part.dtype)
            bwd_b(g).start()

    def finish(g):
        @pl.when(has_a_out)
        def _():
            bwd_a(g).wait_recv()
            own[g] = own[g] + back[A, g].astype(jnp.float32)
        @pl.when(has_b_out)
        def _():
            bwd_b(g).wait_recv()
            own[g] = own[g] + back[B, g].astype(jnp.float32)
        gk_ref[:, cols(g)] = own[g, 0].astype(gk_ref.dtype)
        gv_ref[:, cols(g)] = own[g, 1].astype(gv_ref.dtype)

    relay(0)
    for g in range(heads):
        if g + 1 < heads:
            relay(g + 1)
        arrive(g)
        compute(g)
        give_back(g)
        if g >= 1:
            collect(g - 1)
        if g >= 2:
            finish(g - 2)
    collect(heads - 1)
    for g in range(max(heads - 2, 0), heads):
        finish(g)

    for g in range(heads):
        for cond, copies in (
            (has_a_out, (fwd_a,)), (has_b_out, (fwd_b,)), (has_c, (fwd_c_out, bwd_c)),
            (has_d_out, (fwd_d,)), (has_a_in, (bwd_a,)), (has_b_in, (bwd_b,)), (has_d_in, (bwd_d,)),
        ):
            @pl.when(cond)
            def _():
                for f in copies:
                    f(g).wait_send()


def put_out(*refs):
    sems = refs[-1]
    copies = [
        pltpu.make_async_copy(refs[t], refs[4 + t], sems.at[t]) for t in range(4)
    ]
    for c in copies:
        c.start()
    for c in copies:
        c.wait()


def shards(doc_lengths, queries, key_states, value_head_states, out_grad):
    tok = queries.shape[0]
    heads = key_states.shape[1] // HEAD
    q_heads = queries.shape[1] // HEAD
    n = lax.axis_size("cp")
    window = (REACH + 1) * tok
    bf16, f32 = jnp.bfloat16, jnp.float32
    hbm_spec = pl.BlockSpec(memory_space=pltpu.HBM)
    any_spec = pl.BlockSpec(memory_space=pl.ANY)
    dma = pltpu.SemaphoreType.DMA
    args = [
        pltpu.with_memory_space_constraint(x, pltpu.HBM)
        for x in (doc_lengths, queries, key_states, value_head_states, out_grad)
    ]
    outs = pl.pallas_call(
        functools.partial(kernel, n, doc_lengths.shape[0]),
        out_shape=[
            jax.ShapeDtypeStruct(queries.shape, bf16),
            jax.ShapeDtypeStruct(queries.shape, bf16),
            jax.ShapeDtypeStruct(key_states.shape, bf16),
            jax.ShapeDtypeStruct(key_states.shape, bf16),
        ],
        in_specs=[hbm_spec] * 5,
        out_specs=[pl.BlockSpec(memory_space=pltpu.VMEM)] * 4,
        scratch_shapes=[
            pltpu.VMEM((heads, 2, window, HEAD), bf16),
            pltpu.VMEM((q_heads, tok, HEAD), bf16),
            pltpu.VMEM((q_heads, tok, HEAD), bf16),
            pltpu.VMEM((heads, 2, tok, HEAD), f32),
            pltpu.VMEM((heads, 2, tok, HEAD), f32),
            pltpu.VMEM((heads, 2, REACH * tok, HEAD), bf16),
            pltpu.VMEM((4, heads, 2, tok, HEAD), bf16),
            pltpu.VMEM((window, tok), f32),
            pltpu.SMEM(doc_lengths.shape, jnp.int32),
            dma(()),
            dma((heads, 2)),
            dma((2, q_heads)),
            dma((4, heads)),
            dma((4, heads)),
            dma((4, heads)),
            dma((4, heads)),
        ],
        compiler_params=pltpu.CompilerParams(
            collective_id=0, has_side_effects=True, vmem_limit_bytes=24 * 2**20),
        name="attend",
    )(*args)
    return tuple(pl.pallas_call(
        put_out,
        out_shape=[jax.ShapeDtypeStruct(x.shape, x.dtype) for x in outs],
        in_specs=[any_spec] * 4,
        out_specs=[hbm_spec] * 4,
        scratch_shapes=[dma((4,))],
        compiler_params=pltpu.CompilerParams(vmem_limit_bytes=2**20),
        name="put_out",
    )(*outs))


def solution(mesh):
    wide = P(("group", "cp"), "hd")
    return jax.shard_map(
        shards,
        mesh=mesh,
        in_specs=(P("group"), wide, wide, wide, wide),
        out_specs=(wide, wide, wide, wide),
        check_vma=False,
    )
```

```python
import functools
import math

import jax
import jax.numpy as jnp
from jax import lax
from jax.experimental import pallas as pl
from jax.experimental.pallas import tpu as pltpu
from jax.sharding import PartitionSpec as P

HEAD = 128
REACH = 3
MASKED = -1e30
MESH = pl.DeviceIdType.MESH
X, B, T = range(3)


def kernel(
    n, docs, doc_hbm, q_hbm, k_hbm, v_hbm, do_hbm, o_ref, gq_ref, gk_ref, gv_ref,
    kv, qb, db, own, mid, part, back, bias, doc_ref,
    doc_sem, kv_sem, q_sem, fs_sem, fr_sem, bs_sem, br_sem,
):
    tok = q_hbm.shape[0]
    heads = k_hbm.shape[1] // HEAD
    group = q_hbm.shape[1] // k_hbm.shape[1]
    me = lax.axis_index("cp")
    odd = lax.rem(me, 2)
    is_odd = odd == 1
    is_even = odd == 0
    partner = me + 1 - 2 * odd
    own_rows = pl.ds(REACH * tok, tok)

    def rows(dist):
        return pl.ds((REACH - dist) * tok, tok)

    def cols(h):
        return pl.ds(h * HEAD, HEAD)

    doc_load = pltpu.make_async_copy(doc_hbm, doc_ref, doc_sem)
    doc_load.start()
    kv_loads = []
    for g in range(heads):
        kv_loads.append([
            pltpu.make_async_copy(src.at[:, cols(g)], kv.at[g, t, own_rows], kv_sem.at[g, t])
            for t, src in enumerate((k_hbm, v_hbm))
        ])
        for c in kv_loads[g]:
            c.start()
    q_loads = []
    for h in range(heads * group):
        q_loads.append([
            pltpu.make_async_copy(q_hbm.at[:, cols(h)], qb.at[h], q_sem.at[0, h]),
            pltpu.make_async_copy(do_hbm.at[:, cols(h)], db.at[h], q_sem.at[1, h]),
        ])
        for c in q_loads[h]:
            c.start()

    barrier = pltpu.get_barrier_semaphore()
    for to, cond in ((me - 2, me >= 2), (me + 2, me + 2 < n), (partner, me >= 0)):
        @pl.when(cond)
        def _():
            pl.semaphore_signal(barrier, inc=1, device_id={"cp": to}, device_id_type=MESH)
    pl.semaphore_wait(
        barrier, 1 + jnp.minimum(me // 2, 1) + jnp.minimum((n - 1 - me) // 2, 1))

    def fwd(kind, g, src_rows, dst_rows, to):
        return pltpu.make_async_remote_copy(
            src_ref=kv.at[g, :, src_rows], dst_ref=kv.at[g, :, dst_rows],
            send_sem=fs_sem.at[kind, g], recv_sem=fr_sem.at[kind, g],
            device_id={"cp": to}, device_id_type=MESH,
        )

    def fwd_x(g):
        return fwd(X, g, pl.ds((REACH - 2 * odd) * tok, tok), rows(1), partner)

    def fwd_b(g):
        return fwd(B, g, own_rows, rows(2), me + 2)

    def fwd_t(g):
        return fwd(T, g, rows(1), rows(3), me + 2)

    ahead = me + 2 < n
    behind = me >= 2
    x_in = is_odd | (me >= 2)
    x_out = is_even | (me >= 3)
    t_out = ahead & (me >= 1)
    t_in = me >= 3

    for g in range(heads):
        for c in kv_loads[g]:
            c.wait()
        @pl.when(ahead)
        def _():
            fwd_b(g).start()
        @pl.when(is_even)
        def _():
            fwd_x(g).start()

    for dist in range(1, REACH + 1):
        @pl.when(me < dist)
        def _():
            kv[:, :, (REACH - dist) * tok:(REACH - dist + 1) * tok, :] = jnp.zeros(
                (heads, 2, tok, HEAD), kv.dtype)

    window = (REACH + 1) * tok
    key_pos = (me - REACH) * tok + lax.broadcasted_iota(jnp.int32, (window, tok), 0)
    query_pos = me * tok + lax.broadcasted_iota(jnp.int32, (window, tok), 1)

    doc_load.wait()
    end = jnp.int32(0)
    crossed = jnp.zeros((window, tok), jnp.int32)
    def count(d, carry):
        end, crossed = carry
        end = end + doc_ref[d]
        return end, crossed + jnp.where((key_pos < end) & (query_pos >= end), 1, 0)
    if docs <= 8:
        for d in range(docs):
            end, crossed = count(d, (end, crossed))
    else:
        end, crossed = lax.fori_loop(0, docs, count, (end, crossed))
    allowed = (crossed == 0) & (key_pos <= query_pos) & (key_pos >= 0)
    bias[...] = jnp.where(allowed, 0.0, MASKED)

    def relay_x(g):
        @pl.when(behind)
        def _():
            fwd_b(g).wait_recv()
        @pl.when(is_odd & (me >= 3))
        def _():
            fwd_x(g).start()

    def relay_t(g):
        @pl.when(x_in)
        def _():
            fwd_x(g).wait_recv()
        @pl.when(t_out)
        def _():
            fwd_t(g).start()

    def arrive(g):
        @pl.when(t_in)
        def _():
            fwd_t(g).wait_recv()

    def bwd(kind, g, src_rows, to):
        return pltpu.make_async_remote_copy(
            src_ref=part.at[g, :, src_rows], dst_ref=back.at[kind, g],
            send_sem=bs_sem.at[kind, g], recv_sem=br_sem.at[kind, g],
            device_id={"cp": to}, device_id_type=MESH,
        )

    def bwd_x(g):
        return bwd(X, g, rows(1), partner)

    def bwd_b(g):
        return bwd(B, g, rows(2), me - 2)

    def bwd_t(g):
        return bwd(T, g, rows(3), me - 2)

    score_scale = 1.0 / math.sqrt(HEAD)
    exp_scale = score_scale * math.log2(math.e)
    nt = (((1,), (1,)), ((), ()))
    step = 2 if group % 2 == 0 else 1
    width = step * tok

    def compute(g):
        keys = kv[g, 0]
        values = kv[g, 1]
        keys_t = keys.T
        values_t = values.T
        grad_k = jnp.zeros((window, HEAD), jnp.float32)
        grad_v = jnp.zeros((window, HEAD), jnp.float32)
        mask = jnp.concatenate([bias[...]] * step, axis=1)
        for s in range(group // step):
            h0 = g * group + s * step
            for h in range(h0, h0 + step):
                for c in q_loads[h]:
                    c.wait()
            qs = qb[h0:h0 + step].reshape(width, HEAD)
            ds = db[h0:h0 + step].reshape(width, HEAD)
            scores = lax.dot_general(keys, qs, nt, preferred_element_type=jnp.float32) + mask
            top = jnp.max(scores, axis=0, keepdims=True)
            raw = jnp.exp2((scores - top) * exp_scale)
            probs = raw * (1.0 / jnp.sum(raw, axis=0, keepdims=True))
            low = probs.astype(jnp.bfloat16)
            att_t = jnp.dot(values_t, low, preferred_element_type=jnp.float32)
            grad_p = lax.dot_general(values, ds, nt, preferred_element_type=jnp.float32)
            delta = jnp.sum(probs * grad_p, axis=0, keepdims=True)
            grad_s = (probs * (grad_p - delta)).astype(jnp.bfloat16)
            grad_v = grad_v + jnp.dot(low, ds, preferred_element_type=jnp.float32)
            grad_k = grad_k + jnp.dot(grad_s, qs, preferred_element_type=jnp.float32)
            gq_t = jnp.dot(keys_t, grad_s, preferred_element_type=jnp.float32) * score_scale
            for j in range(step):
                h = h0 + j
                o_ref[:, cols(h)] = att_t[:, j * tok:(j + 1) * tok].T.astype(o_ref.dtype)
                gq_ref[:, cols(h)] = gq_t[:, j * tok:(j + 1) * tok].T.astype(gq_ref.dtype)
        for t, grad in enumerate((grad_k * score_scale, grad_v)):
            part[g, t] = grad[:REACH * tok].astype(part.dtype)
            mid[g, t] = grad[tok:REACH * tok]
            own[g, t] = grad[REACH * tok:]

    def back_t(g):
        @pl.when(t_in)
        def _():
            bwd_t(g).start()

    def back_x(g):
        @pl.when(t_out)
        def _():
            bwd_t(g).wait_recv()
            part[g, :, 2 * tok:] = (
                mid[g, :, tok:] + back[T, g].astype(jnp.float32)).astype(part.dtype)
        @pl.when(x_in)
        def _():
            bwd_x(g).start()

    def back_b(g):
        @pl.when(x_out)
        def _():
            bwd_x(g).wait_recv()
        @pl.when(is_even)
        def _():
            own[g] = own[g] + back[X, g].astype(jnp.float32)
        @pl.when(is_odd & (me >= 3))
        def _():
            part[g, :, tok:2 * tok] = (
                mid[g, :, :tok] + back[X, g].astype(jnp.float32)).astype(part.dtype)
        @pl.when(behind)
        def _():
            bwd_b(g).start()

    def finish(g):
        @pl.when(ahead)
        def _():
            bwd_b(g).wait_recv()
            own[g] = own[g] + back[B, g].astype(jnp.float32)
        gk_ref[:, cols(g)] = own[g, 0].astype(gk_ref.dtype)
        gv_ref[:, cols(g)] = own[g, 1].astype(gv_ref.dtype)

    relay_x(0)
    if heads > 1:
        relay_x(1)
    relay_t(0)
    for g in range(heads + REACH):
        if g < heads:
            if g + 2 < heads:
                relay_x(g + 2)
            if g + 1 < heads:
                relay_t(g + 1)
            arrive(g)
            compute(g)
            back_t(g)
        for lag, stage in enumerate((back_x, back_b, finish)):
            if 0 <= g - 1 - lag < heads:
                stage(g - 1 - lag)

    for g in range(heads):
        for cond, copies in (
            (ahead, (fwd_b,)), (x_out, (fwd_x,)), (t_out, (fwd_t,)),
            (behind, (bwd_b,)), (x_in, (bwd_x,)), (t_in, (bwd_t,)),
        ):
            @pl.when(cond)
            def _():
                for f in copies:
                    f(g).wait_send()


def put_out(*refs):
    sems = refs[-1]
    copies = [
        pltpu.make_async_copy(refs[t], refs[4 + t], sems.at[t]) for t in range(4)
    ]
    for c in copies:
        c.start()
    for c in copies:
        c.wait()


def shards(doc_lengths, queries, key_states, value_head_states, out_grad):
    tok = queries.shape[0]
    heads = key_states.shape[1] // HEAD
    q_heads = queries.shape[1] // HEAD
    n = lax.axis_size("cp")
    window = (REACH + 1) * tok
    bf16, f32 = jnp.bfloat16, jnp.float32
    hbm_spec = pl.BlockSpec(memory_space=pltpu.HBM)
    any_spec = pl.BlockSpec(memory_space=pl.ANY)
    dma = pltpu.SemaphoreType.DMA
    args = [
        pltpu.with_memory_space_constraint(x, pltpu.HBM)
        for x in (doc_lengths, queries, key_states, value_head_states, out_grad)
    ]
    outs = pl.pallas_call(
        functools.partial(kernel, n, doc_lengths.shape[0]),
        out_shape=[
            jax.ShapeDtypeStruct(queries.shape, bf16),
            jax.ShapeDtypeStruct(queries.shape, bf16),
            jax.ShapeDtypeStruct(key_states.shape, bf16),
            jax.ShapeDtypeStruct(key_states.shape, bf16),
        ],
        in_specs=[hbm_spec] * 5,
        out_specs=[pl.BlockSpec(memory_space=pltpu.VMEM)] * 4,
        scratch_shapes=[
            pltpu.VMEM((heads, 2, window, HEAD), bf16),
            pltpu.VMEM((q_heads, tok, HEAD), bf16),
            pltpu.VMEM((q_heads, tok, HEAD), bf16),
            pltpu.VMEM((heads, 2, tok, HEAD), f32),
            pltpu.VMEM((heads, 2, 2 * tok, HEAD), f32),
            pltpu.VMEM((heads, 2, REACH * tok, HEAD), bf16),
            pltpu.VMEM((3, heads, 2, tok, HEAD), bf16),
            pltpu.VMEM((window, tok), f32),
            pltpu.SMEM(doc_lengths.shape, jnp.int32),
            dma(()),
            dma((heads, 2)),
            dma((2, q_heads)),
            dma((3, heads)),
            dma((3, heads)),
            dma((3, heads)),
            dma((3, heads)),
        ],
        compiler_params=pltpu.CompilerParams(
            collective_id=0, has_side_effects=True, vmem_limit_bytes=24 * 2**20),
        name="attend",
    )(*args)
    return tuple(pl.pallas_call(
        put_out,
        out_shape=[jax.ShapeDtypeStruct(x.shape, x.dtype) for x in outs],
        in_specs=[any_spec] * 4,
        out_specs=[hbm_spec] * 4,
        scratch_shapes=[dma((4,))],
        compiler_params=pltpu.CompilerParams(vmem_limit_bytes=2**20),
        name="put_out",
    )(*outs))


def solution(mesh):
    wide = P(("group", "cp"), "hd")
    return jax.shard_map(
        shards,
        mesh=mesh,
        in_specs=(P("group"), wide, wide, wide, wide),
        out_specs=(wide, wide, wide, wide),
        check_vma=False,
    )
```

```python
import functools
import math

import jax
import jax.numpy as jnp
from jax import lax
from jax.experimental import pallas as pl
from jax.experimental.pallas import tpu as pltpu
from jax.sharding import PartitionSpec as P

HEAD = 128
REACH = 3
MASKED = -1e30
MESH = pl.DeviceIdType.MESH
X, B, T = range(3)


def kernel(
    n, docs, doc_hbm, q_hbm, k_hbm, v_hbm, do_hbm, o_ref, gq_ref, gk_ref, gv_ref,
    kv, qb, db, own, mid, part, back, bias, doc_ref,
    doc_sem, kv_sem, q_sem, fs_sem, fr_sem, bs_sem, br_sem,
):
    tok = q_hbm.shape[0]
    heads = k_hbm.shape[1] // HEAD
    group = q_hbm.shape[1] // k_hbm.shape[1]
    me = lax.axis_index("cp")
    odd = lax.rem(me, 2)
    is_odd = odd == 1
    is_even = odd == 0
    partner = me + 1 - 2 * odd
    own_rows = pl.ds(REACH * tok, tok)

    def rows(dist):
        return pl.ds((REACH - dist) * tok, tok)

    def cols(h):
        return pl.ds(h * HEAD, HEAD)

    doc_load = pltpu.make_async_copy(doc_hbm, doc_ref, doc_sem)
    doc_load.start()
    kv_loads = []
    for g in range(heads):
        kv_loads.append([
            pltpu.make_async_copy(src.at[:, cols(g)], kv.at[g, t, own_rows], kv_sem.at[g, t])
            for t, src in enumerate((k_hbm, v_hbm))
        ])
        for c in kv_loads[g]:
            c.start()
    q_loads = []
    for h in range(heads * group):
        q_loads.append([
            pltpu.make_async_copy(q_hbm.at[:, cols(h)], qb.at[h], q_sem.at[0, h]),
            pltpu.make_async_copy(do_hbm.at[:, cols(h)], db.at[h], q_sem.at[1, h]),
        ])
        for c in q_loads[h]:
            c.start()

    barrier = pltpu.get_barrier_semaphore()
    for to, cond in ((me - 2, me >= 2), (me + 2, me + 2 < n), (partner, me >= 0)):
        @pl.when(cond)
        def _():
            pl.semaphore_signal(barrier, inc=1, device_id={"cp": to}, device_id_type=MESH)
    pl.semaphore_wait(
        barrier, 1 + jnp.minimum(me // 2, 1) + jnp.minimum((n - 1 - me) // 2, 1))

    def fwd(kind, g, src_rows, dst_rows, to):
        return pltpu.make_async_remote_copy(
            src_ref=kv.at[g, :, src_rows], dst_ref=kv.at[g, :, dst_rows],
            send_sem=fs_sem.at[kind, g], recv_sem=fr_sem.at[kind, g],
            device_id={"cp": to}, device_id_type=MESH,
        )

    def fwd_x(g):
        return fwd(X, g, pl.ds((REACH - 2 * odd) * tok, tok), rows(1), partner)

    def fwd_b(g):
        return fwd(B, g, own_rows, rows(2), me + 2)

    def fwd_t(g):
        return fwd(T, g, rows(1), rows(3), me + 2)

    ahead = me + 2 < n
    behind = me >= 2
    x_in = is_odd | (me >= 2)
    x_out = is_even | (me >= 3)
    t_out = ahead & (me >= 1)
    t_in = me >= 3

    for g in range(heads):
        for c in kv_loads[g]:
            c.wait()
        @pl.when(ahead)
        def _():
            fwd_b(g).start()
        @pl.when(is_even)
        def _():
            fwd_x(g).start()

    for dist in range(1, REACH + 1):
        @pl.when(me < dist)
        def _():
            kv[:, :, (REACH - dist) * tok:(REACH - dist + 1) * tok, :] = jnp.zeros(
                (heads, 2, tok, HEAD), kv.dtype)

    window = (REACH + 1) * tok
    key_pos = (me - REACH) * tok + lax.broadcasted_iota(jnp.int32, (window, tok), 0)
    query_pos = me * tok + lax.broadcasted_iota(jnp.int32, (window, tok), 1)

    doc_load.wait()
    end = jnp.int32(0)
    crossed = jnp.zeros((window, tok), jnp.int32)
    def count(d, carry):
        end, crossed = carry
        end = end + doc_ref[d]
        return end, crossed + jnp.where((key_pos < end) & (query_pos >= end), 1, 0)
    if docs <= 8:
        for d in range(docs):
            end, crossed = count(d, (end, crossed))
    else:
        end, crossed = lax.fori_loop(0, docs, count, (end, crossed))
    allowed = (crossed == 0) & (key_pos <= query_pos) & (key_pos >= 0)
    bias[...] = jnp.where(allowed, 0.0, MASKED)

    def relay_x(g):
        @pl.when(behind)
        def _():
            fwd_b(g).wait_recv()
        @pl.when(is_odd & (me >= 3))
        def _():
            fwd_x(g).start()

    def relay_t(g):
        @pl.when(x_in)
        def _():
            fwd_x(g).wait_recv()
        @pl.when(t_out)
        def _():
            fwd_t(g).start()

    def arrive(g):
        @pl.when(t_in)
        def _():
            fwd_t(g).wait_recv()

    def bwd(kind, g, src_rows, to):
        return pltpu.make_async_remote_copy(
            src_ref=part.at[g, :, src_rows], dst_ref=back.at[kind, g],
            send_sem=bs_sem.at[kind, g], recv_sem=br_sem.at[kind, g],
            device_id={"cp": to}, device_id_type=MESH,
        )

    def bwd_x(g):
        return bwd(X, g, rows(1), partner)

    def bwd_b(g):
        return bwd(B, g, rows(2), me - 2)

    def bwd_t(g):
        return bwd(T, g, rows(3), me - 2)

    score_scale = 1.0 / math.sqrt(HEAD)
    exp_scale = score_scale * math.log2(math.e)
    nt = (((1,), (1,)), ((), ()))
    step = 2 if group % 2 == 0 else 1
    width = step * tok

    def compute(g):
        keys = kv[g, 0]
        values = kv[g, 1]
        keys_t = keys.T
        values_t = values.T
        grad_k = jnp.zeros((window, HEAD), jnp.float32)
        grad_v = jnp.zeros((window, HEAD), jnp.float32)
        mask = jnp.concatenate([bias[...]] * step, axis=1)
        for s in range(group // step):
            h0 = g * group + s * step
            for h in range(h0, h0 + step):
                for c in q_loads[h]:
                    c.wait()
            qs = qb[h0:h0 + step].reshape(width, HEAD)
            ds = db[h0:h0 + step].reshape(width, HEAD)
            scores = lax.dot_general(keys, qs, nt, preferred_element_type=jnp.float32) + mask
            top = jnp.max(scores, axis=0, keepdims=True)
            raw = jnp.exp2((scores - top) * exp_scale)
            probs = raw * (1.0 / jnp.sum(raw, axis=0, keepdims=True))
            low = probs.astype(jnp.bfloat16)
            att_t = jnp.dot(values_t, low, preferred_element_type=jnp.float32)
            grad_p = lax.dot_general(values, ds, nt, preferred_element_type=jnp.float32)
            delta = jnp.sum(probs * grad_p, axis=0, keepdims=True)
            grad_s = (probs * (grad_p - delta)).astype(jnp.bfloat16)
            grad_v = grad_v + jnp.dot(low, ds, preferred_element_type=jnp.float32)
            grad_k = grad_k + jnp.dot(grad_s, qs, preferred_element_type=jnp.float32)
            gq_t = jnp.dot(keys_t, grad_s, preferred_element_type=jnp.float32) * score_scale
            for j in range(step):
                h = h0 + j
                o_ref[:, cols(h)] = att_t[:, j * tok:(j + 1) * tok].T.astype(o_ref.dtype)
                gq_ref[:, cols(h)] = gq_t[:, j * tok:(j + 1) * tok].T.astype(gq_ref.dtype)
        for t, grad in enumerate((grad_k * score_scale, grad_v)):
            part[g, t] = grad[:REACH * tok].astype(part.dtype)
            mid[g, t] = grad[tok:REACH * tok]
            own[g, t] = grad[REACH * tok:]

    def back_t(g):
        @pl.when(t_in)
        def _():
            bwd_t(g).start()
        @pl.when(is_even & behind)
        def _():
            bwd_b(g).start()

    def back_x(g):
        @pl.when(t_out)
        def _():
            bwd_t(g).wait_recv()
            part[g, :, 2 * tok:] = (
                mid[g, :, tok:] + back[T, g].astype(jnp.float32)).astype(part.dtype)
        @pl.when(x_in)
        def _():
            bwd_x(g).start()

    def back_b(g):
        @pl.when(is_odd & (me >= 3))
        def _():
            bwd_x(g).wait_recv()
            part[g, :, tok:2 * tok] = (
                mid[g, :, :tok] + back[X, g].astype(jnp.float32)).astype(part.dtype)
            bwd_b(g).start()

    def finish(g):
        @pl.when(is_even)
        def _():
            bwd_x(g).wait_recv()
            own[g] = own[g] + back[X, g].astype(jnp.float32)
        @pl.when(ahead)
        def _():
            bwd_b(g).wait_recv()
            own[g] = own[g] + back[B, g].astype(jnp.float32)
        gk_ref[:, cols(g)] = own[g, 0].astype(gk_ref.dtype)
        gv_ref[:, cols(g)] = own[g, 1].astype(gv_ref.dtype)

    relay_x(0)
    if heads > 1:
        relay_x(1)
    relay_t(0)
    for g in range(heads + REACH):
        if g < heads:
            if g + 2 < heads:
                relay_x(g + 2)
            if g + 1 < heads:
                relay_t(g + 1)
            arrive(g)
            compute(g)
            back_t(g)
        for lag, stage in enumerate((back_x, back_b, finish)):
            if 0 <= g - 1 - lag < heads:
                stage(g - 1 - lag)

    for g in range(heads):
        for cond, copies in (
            (ahead, (fwd_b,)), (x_out, (fwd_x,)), (t_out, (fwd_t,)),
            (behind, (bwd_b,)), (x_in, (bwd_x,)), (t_in, (bwd_t,)),
        ):
            @pl.when(cond)
            def _():
                for f in copies:
                    f(g).wait_send()


def put_out(*refs):
    sems = refs[-1]
    copies = [
        pltpu.make_async_copy(refs[t], refs[4 + t], sems.at[t]) for t in range(4)
    ]
    for c in copies:
        c.start()
    for c in copies:
        c.wait()


def shards(doc_lengths, queries, key_states, value_head_states, out_grad):
    tok = queries.shape[0]
    heads = key_states.shape[1] // HEAD
    q_heads = queries.shape[1] // HEAD
    n = lax.axis_size("cp")
    window = (REACH + 1) * tok
    bf16, f32 = jnp.bfloat16, jnp.float32
    hbm_spec = pl.BlockSpec(memory_space=pltpu.HBM)
    any_spec = pl.BlockSpec(memory_space=pl.ANY)
    dma = pltpu.SemaphoreType.DMA
    args = [
        pltpu.with_memory_space_constraint(x, pltpu.HBM)
        for x in (doc_lengths, queries, key_states, value_head_states, out_grad)
    ]
    outs = pl.pallas_call(
        functools.partial(kernel, n, doc_lengths.shape[0]),
        out_shape=[
            jax.ShapeDtypeStruct(queries.shape, bf16),
            jax.ShapeDtypeStruct(queries.shape, bf16),
            jax.ShapeDtypeStruct(key_states.shape, bf16),
            jax.ShapeDtypeStruct(key_states.shape, bf16),
        ],
        in_specs=[hbm_spec] * 5,
        out_specs=[pl.BlockSpec(memory_space=pltpu.VMEM)] * 4,
        scratch_shapes=[
            pltpu.VMEM((heads, 2, window, HEAD), bf16),
            pltpu.VMEM((q_heads, tok, HEAD), bf16),
            pltpu.VMEM((q_heads, tok, HEAD), bf16),
            pltpu.VMEM((heads, 2, tok, HEAD), f32),
            pltpu.VMEM((heads, 2, 2 * tok, HEAD), f32),
            pltpu.VMEM((heads, 2, REACH * tok, HEAD), bf16),
            pltpu.VMEM((3, heads, 2, tok, HEAD), bf16),
            pltpu.VMEM((window, tok), f32),
            pltpu.SMEM(doc_lengths.shape, jnp.int32),
            dma(()),
            dma((heads, 2)),
            dma((2, q_heads)),
            dma((3, heads)),
            dma((3, heads)),
            dma((3, heads)),
            dma((3, heads)),
        ],
        compiler_params=pltpu.CompilerParams(
            collective_id=0, has_side_effects=True, vmem_limit_bytes=24 * 2**20),
        name="attend",
    )(*args)
    return tuple(pl.pallas_call(
        put_out,
        out_shape=[jax.ShapeDtypeStruct(x.shape, x.dtype) for x in outs],
        in_specs=[any_spec] * 4,
        out_specs=[hbm_spec] * 4,
        scratch_shapes=[dma((4,))],
        compiler_params=pltpu.CompilerParams(vmem_limit_bytes=2**20),
        name="put_out",
    )(*outs))


def solution(mesh):
    wide = P(("group", "cp"), "hd")
    return jax.shard_map(
        shards,
        mesh=mesh,
        in_specs=(P("group"), wide, wide, wide, wide),
        out_specs=(wide, wide, wide, wide),
        check_vma=False,
    )
```
